32 devices in a mesh: cluster: 4 (over y, x), member: 8 (over z, core).
Axes of the slice: x: 2, y: 2, z: 4, core: 2. Of those that a mesh axis runs over, the one named last changes fastest.
Arguments:
- embeddings: bfloat16 [8192, 4096], P(('cluster', 'member')), may hold values from -15 to 15, as said below
- start_basis: bfloat16 [4096, 512], P(('cluster', 'member')), may hold values from -6 to 6
- cluster_ids: int32 [8192], P(('cluster', 'member')), may hold values from 0 to 7
- valid_counts: int32 [4], P('cluster'), may hold values from 512 to 2048
Outputs:
- subspace: float32 [4096, 512], P(('cluster', 'member'))
- nearest: float32 [8192], P(('cluster', 'member'))
The draws below stay inside these ranges and needn't reach their ends.
Inputs may be any that keep to these rules, and one draw needn't show every extreme that they name: `embeddings`: Real-valued entries.
All inputs are finite; a program needn't handle non-finite values.
Results may differ from the reference program's by a relative error of at most 0.0042.
Values may be sent and summed in bfloat16 or wider, within the bound.
No kernel may reach another device: no remote copies, remote signals or barrier semaphores. Data moves between devices by JAX's collectives and lax.ppermute only.
A program may use at most 64 MiB of HBM per device.

```python
import math
import jax
import jax.numpy as jnp
from jax import lax

D = 4096
K = 512
ITERS = 2
LABELS = 8
GROUP_ROWS = 2048
GROUPS = 4
ROWS = 8192


def draw_embeddings(key, part):
    first_key, second_key = jax.random.split(key, 2)
    jitter = jnp.clip(jax.random.normal(first_key, (ROWS, D), jnp.float32), -6.0, 6.0)
    common = jnp.clip(jax.random.normal(second_key, (D,), jnp.float32), -4.0, 4.0)
    rising = 0.2 + 0.4 * jnp.arange(ROWS, dtype=jnp.float32) / ROWS
    return (jitter + rising[:, None] * common[None, :]).astype(jnp.bfloat16)


def place_ends(values, own_key, low, top_value):
    longest = values.shape.index(max(values.shape))
    spots = []
    for shift in (0, 1):
        where = [jax.random.randint(jax.random.fold_in(own_key, axis), (), 0, length) for axis, length in enumerate(values.shape)]
        where[longest] = (where[longest] + shift) % values.shape[longest]
        spots.append(tuple(where))
    return values.at[spots[0]].set(low).at[spots[1]].set(top_value)


def block_levels(stream_key, extent, cuts, smallest, high):
    factor_of, own = 1.0, jax.random.fold_in(stream_key, 6)
    for dim, parts in cuts:
        steps = jnp.exp(jax.random.uniform(jax.random.fold_in(own, dim), (parts,), jnp.float32, smallest / len(cuts), high / len(cuts)))
        factor_of = factor_of * jnp.repeat(steps, extent[dim] // parts).reshape([-1 if axis == dim else 1 for axis in range(len(extent))])
    return factor_of


def normal_values(own_key, extent, deviation, most, pieces=(), kind=jnp.bfloat16):
    drawn = deviation * jax.random.normal(own_key, extent, jnp.float32)
    if pieces:
        drawn = drawn * block_levels(own_key, extent, pieces, -0.22, 0.18)
    return jnp.clip(drawn, -most, most).astype(kind)


def setup_inputs(seed: int = 0) -> dict:
    key_list = jax.random.split(jax.random.key(seed), 5)
    return {
        "embeddings": draw_embeddings(jax.random.fold_in(key_list[4], 71), 0),
        "start_basis": normal_values(key_list[1], (D, K), 1.0, 6.0, ((0, 32),)),
        "cluster_ids": place_ends(jax.random.randint(key_list[2], (ROWS,), 0, LABELS), jax.random.fold_in(key_list[2], 1), 0, LABELS - 1).astype(jnp.int32),
        "valid_counts": place_ends(jax.random.randint(key_list[3], (GROUPS,), GROUP_ROWS // 4, GROUP_ROWS + 1), jax.random.fold_in(key_list[3], 1), GROUP_ROWS // 4, GROUP_ROWS).astype(jnp.int32),
    }


EPS = 1e-06

def group_nearest(operands):
    units, labels, limit = operands
    scores = jnp.dot(units.astype(jnp.float32), units.T.astype(jnp.float32), preferred_element_type=jnp.float32)
    position = jnp.arange(units.shape[0], dtype=jnp.int32)
    allowed = (labels[:, None] == labels[None, :]) & (position[None, :] < limit) & (position[None, :] != position[:, None])
    return lax.optimization_barrier(jnp.max(jnp.where(allowed, scores, -1.0), axis=1))

def reference(embeddings, start_basis, cluster_ids, valid_counts):
    total_rows = embeddings.shape[0]
    average = lax.optimization_barrier(jnp.sum(embeddings.astype(jnp.float32), axis=0)) / total_rows
    centered = (embeddings.astype(jnp.float32) - average).astype(jnp.bfloat16)
    basis = start_basis
    orthonormal = None
    for sweep in range(ITERS):
        projected = jnp.dot(centered.astype(jnp.float32), basis.astype(jnp.float32), preferred_element_type=jnp.float32).astype(jnp.bfloat16)
        image = jnp.dot(centered.T.astype(jnp.float32), projected.astype(jnp.float32), preferred_element_type=jnp.float32) / total_rows
        gram = jnp.dot(image.T, image, precision=lax.Precision.HIGHEST)
        lower = jnp.linalg.cholesky(gram)
        orthonormal = jax.scipy.linalg.solve_triangular(lower, image.T, lower=True).T
        basis = orthonormal.astype(jnp.bfloat16)
    subspace = orthonormal * math.sqrt(D)
    coords = jnp.dot(centered.astype(jnp.float32), basis.astype(jnp.float32), preferred_element_type=jnp.float32)
    unit = (coords * lax.rsqrt(lax.optimization_barrier(jnp.sum(coords * coords, axis=1, keepdims=True)) + EPS)).astype(jnp.bfloat16)
    grouped_units = unit.reshape(GROUPS, GROUP_ROWS, K)
    grouped_labels = cluster_ids.reshape(GROUPS, GROUP_ROWS)
    nearest = lax.map(group_nearest, (grouped_units, grouped_labels, valid_counts))
    return (subspace, nearest.reshape(-1))
```

```python
import math

import jax
import jax.numpy as jnp
from jax import lax
from jax.experimental import pallas as pl
from jax.experimental.pallas import tpu as pltpu
from jax.sharding import PartitionSpec as P

D = 4096
ITERS = 2
EPS = 1e-06
HIGHEST = lax.Precision.HIGHEST
F32 = jnp.float32
BF16 = jnp.bfloat16
LANES = 128
GROUP = 16


def matmul(a, b, precision=None):
    return lax.dot_general(a, b, (((1,), (0,)), ((), ())), precision=precision, preferred_element_type=F32)


def matmul_left_t(a, b, precision=None):
    return lax.dot_general(a, b, (((0,), (0,)), ((), ())), precision=precision, preferred_element_type=F32)


def matmul_right_t(a, b, precision=None):
    return lax.dot_general(a, b, (((1,), (1,)), ((), ())), precision=precision, preferred_element_type=F32)


def eliminate_group(rows, at):
    columns = [jnp.broadcast_to(rows[:, at + c : at + c + 1], (GROUP, LANES)) for c in range(GROUP)]
    row_number = lax.broadcasted_iota(jnp.int32, (GROUP, LANES), 0)
    pieces = [rows[:, i * LANES : (i + 1) * LANES] for i in range(rows.shape[1] // LANES)]
    scale = jnp.zeros((GROUP, LANES), F32)
    for c in range(GROUP):
        inverse_root = lax.rsqrt(jnp.broadcast_to(columns[c][c : c + 1, :], (GROUP, LANES)))
        scale = jnp.where(row_number == c, inverse_root, scale)
        if c < GROUP - 1:
            factor = jnp.where(row_number > c, columns[c] * (inverse_root * inverse_root), 0.0)
            for d in range(c + 1, GROUP):
                columns[d] = columns[d] - factor * jnp.broadcast_to(columns[d][c : c + 1, :], (GROUP, LANES))
            pieces = [p - factor * jnp.broadcast_to(p[c : c + 1, :], (GROUP, LANES)) for p in pieces]
    return jnp.concatenate([p * scale for p in pieces], axis=1)


def inverse_cholesky_kernel(gram_ref, out_ref, work_ref, block_ref):
    n = gram_ref.shape[0]
    rows = lax.broadcasted_iota(jnp.int32, (n, n), 0)
    columns = lax.broadcasted_iota(jnp.int32, (n, n), 1)
    work_ref[:, :n] = gram_ref[...]
    work_ref[:, n:] = jnp.where(rows == columns, 1.0, 0.0).astype(F32)
    rows = lax.broadcasted_iota(jnp.int32, (LANES, LANES), 0)
    columns = lax.broadcasted_iota(jnp.int32, (LANES, LANES), 1)
    identity = jnp.where(rows == columns, 1.0, 0.0).astype(F32)
    for lo in range(0, n, LANES):
        hi = lo + LANES
        block_ref[:, :LANES] = work_ref[lo:hi, lo:hi]
        block_ref[:, LANES:] = identity
        for start in range(0, LANES, GROUP):
            end = start + GROUP
            done = eliminate_group(block_ref[start:end, :], start)
            block_ref[start:end, :] = done
            if end < LANES:
                block_ref[end:, :] = block_ref[end:, :] - matmul_left_t(done[:, end:LANES], done, HIGHEST)
        panel = matmul(block_ref[:, LANES:], work_ref[lo:hi, hi : n + hi], HIGHEST)
        if hi < n:
            work_ref[hi:n, hi : n + hi] = work_ref[hi:n, hi : n + hi] - matmul_left_t(panel[:, : n - hi], panel, HIGHEST)
            out_ref[lo:hi, hi:] = jnp.zeros((LANES, n - hi), F32)
        out_ref[lo:hi, :hi] = panel[:, n - hi :]


def inverse_cholesky(gram):
    n = gram.shape[0]
    return pl.pallas_call(
        inverse_cholesky_kernel,
        out_shape=jax.ShapeDtypeStruct((n, n), F32),
        in_specs=[pl.BlockSpec(memory_space=pltpu.VMEM)],
        out_specs=pl.BlockSpec(memory_space=pltpu.VMEM),
        scratch_shapes=[pltpu.VMEM((n, 2 * n), F32), pltpu.VMEM((LANES, 2 * LANES), F32)],
        name="inverse_cholesky",
    )(gram)


def centre_kernel(order_ref, x_ref, average_ref, out_ref):
    for j in range(out_ref.shape[1] // LANES):
        source = pl.ds(pl.multiple_of(order_ref[j] * LANES, LANES), LANES)
        out_ref[:, j * LANES : (j + 1) * LANES] = (x_ref[:, source].astype(F32) - average_ref[:, source]).astype(BF16)


def centre(x, average, order):
    blocks = order.shape[0]
    width = x.shape[1] // blocks
    if width != LANES:
        columns = (order[:, None] * width + jnp.arange(width)).reshape(-1)
        return jnp.take((x.astype(F32) - average).astype(BF16), columns, axis=1)
    return pl.pallas_call(
        centre_kernel,
        out_shape=jax.ShapeDtypeStruct(x.shape, BF16),
        in_specs=[
            pl.BlockSpec(memory_space=pltpu.SMEM),
            pl.BlockSpec(memory_space=pltpu.VMEM),
            pl.BlockSpec(memory_space=pltpu.VMEM),
        ],
        out_specs=pl.BlockSpec(memory_space=pltpu.VMEM),
        name="centre",
    )(order, x, average)


def make_body(n_cluster, n_member):
    cluster_bits = [1 << b for b in range(n_cluster.bit_length() - 1)]
    member_bits = [1 << b for b in range(n_member.bit_length() - 1)]
    core, outer = member_bits[0], member_bits[:0:-1]
    orders = (cluster_bits, cluster_bits[::-1])

    def swap(x, axis, bit):
        size = n_cluster if axis == "cluster" else n_member
        return lax.ppermute(x, axis, [(i, i ^ bit) for i in range(size)])

    def with_bit(numbers, bit):
        return [i ^ bit for i in numbers]

    part = [0]
    for bit in outer[:-1]:
        part = part + with_bit(part, bit)
    parts = [part, with_bit(part, outer[-1])]
    pieces = []
    for numbers, order in zip(parts, orders):
        for bit in order[:-1]:
            numbers = numbers + with_bit(numbers, bit * n_member)
        pieces += [numbers, with_bit(numbers, order[-1] * n_member)]
    pieces = [pieces[0], pieces[2], pieces[1], pieces[3]]
    pieces += [with_bit(p, core) for p in pieces]
    relative = [i for p in pieces for i in p]

    def gather(x):
        for bit in outer[:-1]:
            x = jnp.concatenate([x, swap(x, "member", bit)])
        near, far = [], []
        for y, order in zip((x, swap(x, "member", outer[-1])), orders):
            for bit in order[:-1]:
                y = jnp.concatenate([y, swap(y, "cluster", bit)])
            near.append(y)
            far.append(swap(y, "cluster", order[-1]))
        held = near + far
        return held + [swap(p, "member", core) for p in held]

    def halve(x, axis, bit, kind):
        half = x.shape[0] // 2
        return x[:half] + swap(x[half:].astype(kind), axis, bit).astype(F32)

    def reduce_scatter(products):
        held = [products[i] + swap(products[i + 4], "member", core) for i in range(4)]
        parts = []
        for i, order in enumerate(orders):
            y = held[i] + swap(held[i + 2].astype(BF16), "cluster", order[-1]).astype(F32)
            for bit in order[-2::-1]:
                y = halve(y, "cluster", bit, BF16)
            parts.append(y)
        x = parts[0] + swap(parts[1], "member", outer[-1])
        for bit in outer[-2::-1]:
            x = halve(x, "member", bit, F32)
        return x

    def all_sum(x):
        for axis, bits in (("member", outer + [core]), ("cluster", cluster_bits)):
            for bit in bits:
                x = x + swap(x, axis, bit)
        return x

    def body(embeddings, start_basis, cluster_ids, valid_counts):
        row_count = embeddings.shape[0]
        total_rows = row_count * n_cluster * n_member
        member = lax.axis_index("member")
        own = lax.axis_index("cluster") * n_member + member
        ones_row = jnp.ones((1, row_count), BF16)
        average = all_sum(matmul(ones_row, embeddings)) / total_rows
        centered = centre(embeddings, average, own ^ jnp.array(relative, jnp.int32))
        ends = [0]
        for p in pieces:
            ends.append(ends[-1] + len(p) * start_basis.shape[0])
        centered_pieces = [centered[:, a:b] for a, b in zip(ends[:-1], ends[1:])]

        def project(basis_pieces):
            return sum(matmul(c, b) for c, b in zip(centered_pieces, basis_pieces))

        projected = project(gather(start_basis))
        for sweep in range(ITERS):
            rounded = projected.astype(BF16)
            image = reduce_scatter([matmul_left_t(c, rounded) for c in centered_pieces]) / total_rows
            image_pieces = gather(image.astype(BF16))
            gram = sum(matmul_left_t(p, p) for p in image_pieces)
            inverse = inverse_cholesky(gram)
            projected = matmul_right_t(project(image_pieces), inverse, HIGHEST)
        subspace = matmul_right_t(image, inverse, HIGHEST) * math.sqrt(D)
        coords = projected
        unit = (coords * lax.rsqrt(jnp.sum(coords * coords, axis=1, keepdims=True) + EPS)).astype(BF16)
        position = jnp.arange(row_count, dtype=jnp.int32)
        codes = jnp.where(member * row_count + position < valid_counts[0], cluster_ids, -1)
        for bit in outer + [core]:
            codes = jnp.concatenate([codes, swap(codes, "member", bit)])
        unit_pieces = [unit]
        for bit in outer:
            unit_pieces.append(swap(unit_pieces[0] if len(unit_pieces) == 1 else jnp.concatenate(unit_pieces), "member", bit))
        unit_pieces.append(swap(jnp.concatenate(unit_pieces), "member", core))
        nearest = jnp.full((row_count,), -1.0, F32)
        at = 0
        for i, other in enumerate(unit_pieces):
            scores = matmul_right_t(unit, other)
            allowed = cluster_ids[:, None] == codes[None, at : at + other.shape[0]]
            if i == 0:
                allowed = allowed & (position[:, None] != position[None, :])
            nearest = jnp.maximum(nearest, jnp.max(jnp.where(allowed, scores, -1.0), axis=1))
            at += other.shape[0]
        return (subspace, nearest)

    return body


def solution(mesh):
    rows = ("cluster", "member")
    return jax.shard_map(
        make_body(mesh.shape["cluster"], mesh.shape["member"]),
        mesh=mesh,
        in_specs=(P(rows, None), P(rows, None), P(rows), P("cluster")),
        out_specs=(P(rows, None), P(rows)),
        check_vma=False,
    )
```

```python
import math

import jax
import jax.numpy as jnp
from jax import lax
from jax.experimental import pallas as pl
from jax.experimental.pallas import tpu as pltpu
from jax.sharding import PartitionSpec as P

D = 4096
ITERS = 2
EPS = 1e-06
HIGHEST = lax.Precision.HIGHEST
F32 = jnp.float32
BF16 = jnp.bfloat16
LANES = 128
GROUP = 16
SPLIT = 1
LOOP = False


def matmul(a, b, precision=None):
    return lax.dot_general(a, b, (((1,), (0,)), ((), ())), precision=precision, preferred_element_type=F32)


def matmul_left_t(a, b, precision=None):
    return lax.dot_general(a, b, (((0,), (0,)), ((), ())), precision=precision, preferred_element_type=F32)


def matmul_right_t(a, b, precision=None):
    return lax.dot_general(a, b, (((1,), (1,)), ((), ())), precision=precision, preferred_element_type=F32)


def eliminate_group(rows, at):
    columns = [jnp.broadcast_to(rows[:, at + c : at + c + 1], (GROUP, LANES)) for c in range(GROUP)]
    row_number = lax.broadcasted_iota(jnp.int32, (GROUP, LANES), 0)
    pieces = [rows[:, i * LANES : (i + 1) * LANES] for i in range(rows.shape[1] // LANES)]
    scale = jnp.zeros((GROUP, LANES), F32)
    for c in range(GROUP):
        inverse_root = lax.rsqrt(jnp.broadcast_to(columns[c][c : c + 1, :], (GROUP, LANES)))
        scale = jnp.where(row_number == c, inverse_root, scale)
        if c < GROUP - 1:
            factor = jnp.where(row_number > c, columns[c] * (inverse_root * inverse_root), 0.0)
            for d in range(c + 1, GROUP):
                columns[d] = columns[d] - factor * jnp.broadcast_to(columns[d][c : c + 1, :], (GROUP, LANES))
            pieces = [p - factor * jnp.broadcast_to(p[c : c + 1, :], (GROUP, LANES)) for p in pieces]
    return jnp.concatenate([p * scale for p in pieces], axis=1)


def inverse_cholesky_kernel(*refs):
    *gram_refs, out_ref, work_ref, block_ref = refs
    n = out_ref.shape[0]
    rows = lax.broadcasted_iota(jnp.int32, (n, n), 0)
    columns = lax.broadcasted_iota(jnp.int32, (n, n), 1)
    count = round(math.sqrt(2 * len(gram_refs)))
    side = n // count
    blocks = iter(gram_refs)
    for i in range(count):
        for j in range(i, count):
            work_ref[i * side : (i + 1) * side, j * side : (j + 1) * side] = next(blocks)[...]
        for j in range(i):
            work_ref[i * side : (i + 1) * side, j * side : (j + 1) * side] = jnp.zeros((side, side), F32)
    work_ref[:, n:] = jnp.where(rows == columns, 1.0, 0.0).astype(F32)

    def step(k, carry):
        at = pl.multiple_of(k * LANES, LANES)
        rows = lax.broadcasted_iota(jnp.int32, (LANES, LANES), 0)
        columns = lax.broadcasted_iota(jnp.int32, (LANES, LANES), 1)
        block_ref[:, :LANES] = work_ref[pl.ds(at, LANES), pl.ds(at, LANES)]
        block_ref[:, LANES:] = jnp.where(rows == columns, 1.0, 0.0).astype(F32)
        for start in range(0, LANES, GROUP):
            end = start + GROUP
            done = eliminate_group(block_ref[start:end, :], start)
            block_ref[start:end, :] = done
            if end < LANES:
                block_ref[end:, :] = block_ref[end:, :] - matmul_left_t(done[:, end:LANES], done, HIGHEST)
        for lo in range(0, n, LANES):
            pl.when(k == lo // LANES)(lambda lo=lo: spread(lo))
        return carry

    def spread(lo):
        hi = lo + LANES
        panel = matmul(block_ref[:, LANES:], work_ref[lo:hi, hi : n + hi], HIGHEST)
        if hi < n:
            work_ref[hi:n, hi : n + hi] = work_ref[hi:n, hi : n + hi] - matmul_left_t(panel[:, : n - hi], panel, HIGHEST)
            out_ref[lo:hi, hi:] = jnp.zeros((LANES, n - hi), F32)
        out_ref[lo:hi, :hi] = panel[:, n - hi :]

    lax.fori_loop(0, n // LANES, step, 0)


def inverse_cholesky(n, gram_blocks):
    return pl.pallas_call(
        inverse_cholesky_kernel,
        out_shape=jax.ShapeDtypeStruct((n, n), F32),
        in_specs=[pl.BlockSpec(memory_space=pltpu.VMEM)] * len(gram_blocks),
        out_specs=pl.BlockSpec(memory_space=pltpu.VMEM),
        scratch_shapes=[pltpu.VMEM((n, 2 * n), F32), pltpu.VMEM((LANES, 2 * LANES), F32)],
        name="inverse_cholesky",
    )(*gram_blocks)


def centre_kernel(order_ref, x_ref, average_ref, out_ref):
    for j in range(out_ref.shape[1] // LANES):
        source = pl.ds(pl.multiple_of(order_ref[j] * LANES, LANES), LANES)
        out_ref[:, j * LANES : (j + 1) * LANES] = (x_ref[:, source].astype(F32) - average_ref[:, source]).astype(BF16)


def centre(x, average, order):
    blocks = order.shape[0]
    width = x.shape[1] // blocks
    if width != LANES:
        columns = (order[:, None] * width + jnp.arange(width)).reshape(-1)
        return jnp.take((x.astype(F32) - average).astype(BF16), columns, axis=1)
    return pl.pallas_call(
        centre_kernel,
        out_shape=jax.ShapeDtypeStruct(x.shape, BF16),
        in_specs=[
            pl.BlockSpec(memory_space=pltpu.SMEM),
            pl.BlockSpec(memory_space=pltpu.VMEM),
            pl.BlockSpec(memory_space=pltpu.VMEM),
        ],
        out_specs=pl.BlockSpec(memory_space=pltpu.VMEM),
        name="centre",
    )(order, x, average)


def make_body(n_cluster, n_member):
    cluster_bits = [1 << b for b in range(n_cluster.bit_length() - 1)]
    member_bits = [1 << b for b in range(n_member.bit_length() - 1)]
    core = member_bits[0]
    outer = range(2 * core, n_member, 2 * core)
    orders = (cluster_bits, cluster_bits[::-1])

    def swap(x, axis, bit):
        size = n_cluster if axis == "cluster" else n_member
        return lax.ppermute(x, axis, [(i, i ^ bit) for i in range(size)])

    def with_bit(numbers, bit):
        return [i ^ bit for i in numbers]

    blocks = [0, *outer]
    parts = [blocks[: len(blocks) // 2], blocks[len(blocks) // 2 :]]
    pieces = []
    for numbers, order in zip(parts, orders):
        for bit in order[:-1]:
            numbers = numbers + with_bit(numbers, bit * n_member)
        pieces += [numbers, with_bit(numbers, order[-1] * n_member)]
    pieces = [pieces[0], pieces[2], pieces[1], pieces[3]]
    pieces += [with_bit(p, core) for p in pieces]
    relative = [i for p in pieces for i in p]

    def turns(parts, steps):
        results, before = [], None
        for part in parts:
            log = []

            def send(x, axis, bit, before=before, log=log):
                if before is not None:
                    x, _ = lax.optimization_barrier((x, before[len(log)]))
                log.append(swap(x, axis, bit))
                return log[-1]

            results.append(steps(part, send))
            before = log
        return results

    def gather_steps(x, send):
        blocks = [x] + [send(x, "member", other) for other in outer]
        middle = len(blocks) // 2
        parts = [jnp.concatenate(blocks[:middle]), jnp.concatenate(blocks[middle:])]
        for i in range(len(cluster_bits) - 1):
            parts = [jnp.concatenate([y, send(y, "cluster", order[i])]) for y, order in zip(parts, orders)]
        held = parts + [send(y, "cluster", order[-1]) for y, order in zip(parts, orders)]
        return held + [swap(p, "member", core) for p in held]

    def reduce_steps(products, send):
        def halve(x, axis, bit, kind):
            half = x.shape[0] // 2
            return x[:half] + send(x[half:].astype(kind), axis, bit).astype(F32)

        held = [products[i] + swap(products[i + 4], "member", core) for i in range(4)]
        parts = [
            held[i] + send(held[i + 2].astype(BF16), "cluster", order[-1]).astype(F32) for i, order in enumerate(orders)
        ]
        for i in range(len(cluster_bits) - 2, -1, -1):
            parts = [halve(y, "cluster", order[i], BF16) for y, order in zip(parts, orders)]
        rows = parts[0].shape[0] // (len(blocks) // 2)
        own, *others = [y[i : i + rows] for y in parts for i in range(0, y.shape[0], rows)]
        for block, other in zip(others, outer):
            own = own + send(block.astype(BF16), "member", other).astype(F32)
        return own

    def all_sum(x):
        x = sum([swap(x, "cluster", other) for other in range(1, n_cluster)], x)
        x = sum([swap(x, "member", other) for other in outer], x)
        return x + swap(x, "member", core)

    def body(embeddings, start_basis, cluster_ids, valid_counts):
        row_count = embeddings.shape[0]
        total_rows = row_count * n_cluster * n_member
        member = lax.axis_index("member")
        own = lax.axis_index("cluster") * n_member + member
        ones_row = jnp.ones((1, row_count), BF16)
        average = all_sum(matmul(ones_row, embeddings)) / total_rows
        centered = centre(embeddings, average, own ^ jnp.array(relative, jnp.int32))
        ends = [0]
        for p in pieces:
            ends.append(ends[-1] + len(p) * start_basis.shape[0])
        centered_pieces = [centered[:, a:b] for a, b in zip(ends[:-1], ends[1:])]

        width = start_basis.shape[1]
        position = jnp.arange(row_count, dtype=jnp.int32)
        ids, _ = lax.optimization_barrier((cluster_ids, average))
        codes = jnp.where(member * row_count + position < valid_counts[0], ids, -1)
        codes = jnp.concatenate([codes] + [swap(codes, "member", other) for other in outer])
        codes = jnp.concatenate([codes, swap(codes, "member", core)])

        def split(x):
            return [x[:, i * width // SPLIT : (i + 1) * width // SPLIT] for i in range(SPLIT)]

        def project(basis_parts):
            return [sum(matmul(c, b) for c, b in zip(centered_pieces, part)) for part in basis_parts]

        def sweep(_, carry):
            projected = split(carry[0])
            products = [[matmul_left_t(c, r) for c in centered_pieces] for r in projected]
            image = [x / total_rows for x in turns(products, reduce_steps)]
            image_parts = turns([x.astype(BF16) for x in image], gather_steps)
            gram = [
                sum(matmul_left_t(a, b) for a, b in zip(image_parts[i], image_parts[j]))
                for i in range(SPLIT)
                for j in range(i, SPLIT)
            ]
            inverse = inverse_cholesky(width, gram)
            projected = matmul_right_t(jnp.concatenate(project(image_parts), axis=1), inverse, HIGHEST)
            return projected.astype(BF16), projected, jnp.concatenate(image, axis=1), inverse

        projected = jnp.concatenate(project(turns(split(start_basis), gather_steps)), axis=1).astype(BF16)
        projected, codes = lax.optimization_barrier((projected, codes))
        if LOOP:
            empty = (jnp.zeros((row_count, width), F32), jnp.zeros(start_basis.shape, F32), jnp.zeros((width, width), F32))
            carry = lax.fori_loop(0, ITERS, sweep, (projected, *empty))
        else:
            carry = (projected,)
            for i in range(ITERS):
                carry = sweep(i, carry)
        _, projected, image, inverse = carry
        subspace = matmul_right_t(image, inverse, HIGHEST) * math.sqrt(D)
        coords = projected
        unit = (coords * lax.rsqrt(jnp.sum(coords * coords, axis=1, keepdims=True) + EPS)).astype(BF16)
        unit_pieces = [unit] + [swap(unit, "member", other) for other in outer]
        unit_pieces[1], subspace = lax.optimization_barrier((unit_pieces[1], subspace))
        unit_pieces += [swap(p, "member", core) for p in unit_pieces]
        nearest = jnp.full((row_count,), -1.0, F32)
        at = 0
        for i, other in enumerate(unit_pieces):
            scores = matmul_right_t(unit, other)
            allowed = cluster_ids[:, None] == codes[None, at : at + other.shape[0]]
            if i == 0:
                allowed = allowed & (position[:, None] != position[None, :])
            nearest = jnp.maximum(nearest, jnp.max(jnp.where(allowed, scores, -1.0), axis=1))
            at += other.shape[0]
        return (subspace, nearest)

    return body


def solution(mesh):
    rows = ("cluster", "member")
    return jax.shard_map(
        make_body(mesh.shape["cluster"], mesh.shape["member"]),
        mesh=mesh,
        in_specs=(P(rows, None), P(rows, None), P(rows), P("cluster")),
        out_specs=(P(rows, None), P(rows)),
        check_vma=False,
    )
```

```python
import math

import jax
import jax.numpy as jnp
from jax import lax
from jax.experimental import pallas as pl
from jax.experimental.pallas import tpu as pltpu
from jax.sharding import PartitionSpec as P

D = 4096
ITERS = 2
EPS = 1e-06
HIGHEST = lax.Precision.HIGHEST
F32 = jnp.float32
BF16 = jnp.bfloat16
LANES = 128
GROUP = 16


def matmul(a, b, precision=None):
    return lax.dot_general(a, b, (((1,), (0,)), ((), ())), precision=precision, preferred_element_type=F32)


def matmul_left_t(a, b, precision=None):
    return lax.dot_general(a, b, (((0,), (0,)), ((), ())), precision=precision, preferred_element_type=F32)


def matmul_right_t(a, b, precision=None):
    return lax.dot_general(a, b, (((1,), (1,)), ((), ())), precision=precision, preferred_element_type=F32)


def eliminate_group(rows, at):
    height = rows.shape[0]
    columns = [jnp.broadcast_to(rows[:, at + c : at + c + 1], (height, LANES)) for c in range(GROUP)]
    row_number = lax.broadcasted_iota(jnp.int32, (height, LANES), 0)
    pieces = [rows[:, i * LANES : (i + 1) * LANES] for i in range(rows.shape[1] // LANES)]
    scale = jnp.zeros((GROUP, LANES), F32)
    for c in range(GROUP):
        inverse_root = lax.rsqrt(jnp.broadcast_to(columns[c][c : c + 1, :], (height, LANES)))
        scale = jnp.where(row_number[:GROUP] == c, inverse_root[:GROUP], scale)
        factor = jnp.where(row_number > c, columns[c] * (inverse_root * inverse_root), 0.0)
        for d in range(c + 1, GROUP):
            columns[d] = columns[d] - factor * jnp.broadcast_to(columns[d][c : c + 1, :], (height, LANES))
        pieces = [p - factor * jnp.broadcast_to(p[c : c + 1, :], (height, LANES)) for p in pieces]
    done = jnp.concatenate([p[:GROUP] * scale for p in pieces], axis=1)
    return done, jnp.concatenate([p[GROUP:] for p in pieces], axis=1)


def inverse_cholesky_kernel(gram_ref, out_ref, work_ref, block_ref):
    n = gram_ref.shape[0]
    rows = lax.broadcasted_iota(jnp.int32, (n, n), 0)
    columns = lax.broadcasted_iota(jnp.int32, (n, n), 1)
    work_ref[:, :n] = gram_ref[...]
    work_ref[:, n:] = jnp.where(rows == columns, 1.0, 0.0).astype(F32)

    def step(k, carry):
        at = pl.multiple_of(k * LANES, LANES)
        rows = lax.broadcasted_iota(jnp.int32, (LANES, LANES), 0)
        columns = lax.broadcasted_iota(jnp.int32, (LANES, LANES), 1)
        block_ref[:, :LANES] = work_ref[pl.ds(at, LANES), pl.ds(at, LANES)]
        block_ref[:, LANES:] = jnp.where(rows == columns, 1.0, 0.0).astype(F32)
        ahead = block_ref[:GROUP, :]
        for start in range(0, LANES, GROUP):
            end = start + GROUP
            rows = ahead if end == LANES else jnp.concatenate([ahead, block_ref[end : end + GROUP, :]], axis=0)
            done, ahead = eliminate_group(rows, start)
            block_ref[start:end, :] = done
            end += GROUP
            if end < LANES:
                block_ref[end:, :] = block_ref[end:, :] - matmul_left_t(done[:, end:LANES], done, HIGHEST)
        for lo in range(0, n, LANES):
            pl.when(k == lo // LANES)(lambda lo=lo: spread(lo))
        return carry

    def spread(lo):
        hi = lo + LANES
        panel = matmul(block_ref[:, LANES:], work_ref[lo:hi, hi : n + hi], HIGHEST)
        if hi < n:
            work_ref[hi:n, hi : n + hi] = work_ref[hi:n, hi : n + hi] - matmul_left_t(panel[:, : n - hi], panel, HIGHEST)
            out_ref[lo:hi, hi:] = jnp.zeros((LANES, n - hi), F32)
        out_ref[lo:hi, :hi] = panel[:, n - hi :]

    lax.fori_loop(0, n // LANES, step, 0)


def inverse_cholesky(gram):
    n = gram.shape[0]
    return pl.pallas_call(
        inverse_cholesky_kernel,
        out_shape=jax.ShapeDtypeStruct((n, n), F32),
        in_specs=[pl.BlockSpec(memory_space=pltpu.VMEM)],
        out_specs=pl.BlockSpec(memory_space=pltpu.VMEM),
        scratch_shapes=[pltpu.VMEM((n, 2 * n), F32), pltpu.VMEM((LANES, 2 * LANES), F32)],
        name="inverse_cholesky",
    )(gram)


def centre_kernel(order_ref, x_ref, average_ref, out_ref):
    for j in range(out_ref.shape[1] // LANES):
        source = pl.ds(pl.multiple_of(order_ref[j] * LANES, LANES), LANES)
        out_ref[:, j * LANES : (j + 1) * LANES] = (x_ref[:, source].astype(F32) - average_ref[:, source]).astype(BF16)


def centre(x, average, order):
    blocks = order.shape[0]
    width = x.shape[1] // blocks
    if width != LANES:
        columns = (order[:, None] * width + jnp.arange(width)).reshape(-1)
        return jnp.take((x.astype(F32) - average).astype(BF16), columns, axis=1)
    return pl.pallas_call(
        centre_kernel,
        out_shape=jax.ShapeDtypeStruct(x.shape, BF16),
        in_specs=[
            pl.BlockSpec(memory_space=pltpu.SMEM),
            pl.BlockSpec(memory_space=pltpu.VMEM),
            pl.BlockSpec(memory_space=pltpu.VMEM),
        ],
        out_specs=pl.BlockSpec(memory_space=pltpu.VMEM),
        name="centre",
    )(order, x, average)


def make_body(n_cluster, n_member):
    cluster_bits = [1 << b for b in range(n_cluster.bit_length() - 1)]
    member_bits = [1 << b for b in range(n_member.bit_length() - 1)]
    core = member_bits[0]
    outer = range(2 * core, n_member, 2 * core)
    orders = (cluster_bits, cluster_bits[::-1])

    def swap(x, axis, bit):
        size = n_cluster if axis == "cluster" else n_member
        return lax.ppermute(x, axis, [(i, i ^ bit) for i in range(size)])

    def with_bit(numbers, bit):
        return [i ^ bit for i in numbers]

    blocks = [0, *outer]
    parts = [blocks[: len(blocks) // 2], blocks[len(blocks) // 2 :]]
    pieces = []
    for numbers, order in zip(parts, orders):
        for bit in order[:-1]:
            numbers = numbers + with_bit(numbers, bit * n_member)
        pieces += [numbers, with_bit(numbers, order[-1] * n_member)]
    pieces = [pieces[0], pieces[2], pieces[1], pieces[3]]
    pieces += [with_bit(p, core) for p in pieces]
    relative = [i for p in pieces for i in p]

    def gather_steps(x, send):
        blocks = [x] + [send(x, "member", other) for other in outer]
        middle = len(blocks) // 2
        parts = [jnp.concatenate(blocks[:middle]), jnp.concatenate(blocks[middle:])]
        for i in range(len(cluster_bits) - 1):
            parts = [jnp.concatenate([y, send(y, "cluster", order[i])]) for y, order in zip(parts, orders)]
        held = parts + [send(y, "cluster", order[-1]) for y, order in zip(parts, orders)]
        return held + [swap(p, "member", core) for p in held]

    def reduce_steps(products, send, held):
        def halve(x, axis, bit, kind):
            half = x.shape[0] // 2
            return x[:half] + send(x[half:].astype(kind), axis, bit).astype(F32)

        held += [products[i] + swap(products[i + 4], "member", core) for i in range(4)]
        parts = [
            held[i] + send(held[i + 2].astype(BF16), "cluster", order[-1]).astype(F32) for i, order in enumerate(orders)
        ]
        for i in range(len(cluster_bits) - 2, -1, -1):
            parts = [halve(y, "cluster", order[i], BF16) for y, order in zip(parts, orders)]
        rows = parts[0].shape[0] // (len(blocks) // 2)
        own, *others = [y[i : i + rows] for y in parts for i in range(0, y.shape[0], rows)]
        for block, other in zip(others, outer):
            own = own + send(block.astype(BF16), "member", other).astype(F32)
        return own

    def all_sum(x, near):
        x = x + swap(x, "member", core)
        x, _ = lax.optimization_barrier((x, near))
        x = sum([swap(x, "member", other) for other in outer], x)
        return sum([swap(x, "cluster", other) for other in range(1, n_cluster)], x)

    def body(embeddings, start_basis, cluster_ids, valid_counts):
        row_count = embeddings.shape[0]
        total_rows = row_count * n_cluster * n_member
        member = lax.axis_index("member")
        own = lax.axis_index("cluster") * n_member + member
        ones_row = jnp.ones((1, row_count), BF16)
        first = []

        def first_send(x, axis, bit):
            first.append(swap(x, axis, bit))
            return first[-1]

        start_pieces = gather_steps(start_basis, first_send)
        average = all_sum(matmul(ones_row, embeddings), first[0]) / total_rows
        average, *_ = lax.optimization_barrier((average, *first[len(outer) : len(outer) + 2]))
        centered = centre(embeddings, average, own ^ jnp.array(relative, jnp.int32))
        ends = [0]
        for p in pieces:
            ends.append(ends[-1] + len(p) * start_basis.shape[0])
        centered_pieces = [centered[:, a:b] for a, b in zip(ends[:-1], ends[1:])]

        position = jnp.arange(row_count, dtype=jnp.int32)

        def label_codes(after):
            ids, _ = lax.optimization_barrier((cluster_ids, after))
            codes = jnp.where(member * row_count + position < valid_counts[0], ids, -1)
            codes = jnp.stack([codes, swap(codes, "member", core)])
            return jnp.stack([codes] + [swap(codes, "member", other) for other in outer])

        def project(basis_pieces):
            return sum(matmul(c, b) for c, b in zip(centered_pieces, basis_pieces))

        projected = project(start_pieces).astype(BF16)
        for sweep in range(ITERS):
            held = []
            products = [matmul_left_t(c, projected) for c in centered_pieces]
            image = reduce_steps(products, swap, held) / total_rows
            image_rounded = image.astype(BF16)
            if sweep == 0:
                image_rounded, codes = lax.optimization_barrier((image_rounded, label_codes(held[0])))
            image_pieces = gather_steps(image_rounded, swap)
            gram = sum(matmul_left_t(p, p) for p in image_pieces)
            inverse = inverse_cholesky(gram)
            coords = matmul_right_t(project(image_pieces), inverse, HIGHEST)
            projected = coords.astype(BF16)
        subspace = matmul_right_t(image, inverse, HIGHEST) * math.sqrt(D)
        unit = (coords * lax.rsqrt(jnp.sum(coords * coords, axis=1, keepdims=True) + EPS)).astype(BF16)
        unit_pieces = [unit] + [swap(unit, "member", other) for other in outer]
        unit_pieces[1], subspace = lax.optimization_barrier((unit_pieces[1], subspace))
        unit_pieces += [swap(p, "member", core) for p in unit_pieces]
        nearest = jnp.full((row_count,), -1.0, F32)
        for i, other in enumerate(unit_pieces):
            scores = matmul_right_t(unit, other)
            across, block = divmod(i, len(blocks))
            allowed = cluster_ids[:, None] == codes[block, across][None, :]
            if i == 0:
                allowed = allowed & (position[:, None] != position[None, :])
            nearest = jnp.maximum(nearest, jnp.max(jnp.where(allowed, scores, -1.0), axis=1))
        return (subspace, nearest)

    return body


def solution(mesh):
    rows = ("cluster", "member")
    return jax.shard_map(
        make_body(mesh.shape["cluster"], mesh.shape["member"]),
        mesh=mesh,
        in_specs=(P(rows, None), P(rows, None), P(rows), P("cluster")),
        out_specs=(P(rows, None), P(rows)),
        check_vma=False,
    )
```

```python
import math

import jax
import jax.numpy as jnp
from jax import lax
from jax.experimental import pallas as pl
from jax.experimental.pallas import tpu as pltpu
from jax.sharding import PartitionSpec as P

D = 4096
ITERS = 2
EPS = 1e-06
HIGHEST = lax.Precision.HIGHEST
F32 = jnp.float32
BF16 = jnp.bfloat16
LANES = 128
GROUP = 16
KERNEL_BYTES = 8 << 20


def matmul(a, b, precision=None):
    return lax.dot_general(a, b, (((1,), (0,)), ((), ())), precision=precision, preferred_element_type=F32)


def matmul_left_t(a, b, precision=None):
    return lax.dot_general(a, b, (((0,), (0,)), ((), ())), precision=precision, preferred_element_type=F32)


def matmul_right_t(a, b, precision=None):
    return lax.dot_general(a, b, (((1,), (1,)), ((), ())), precision=precision, preferred_element_type=F32)


def eliminate_group(rows, at):
    height = rows.shape[0]
    columns = [jnp.broadcast_to(rows[:, at + c : at + c + 1], (height, LANES)) for c in range(GROUP)]
    row_number = lax.broadcasted_iota(jnp.int32, (height, LANES), 0)
    pieces = [rows[:, i * LANES : (i + 1) * LANES] for i in range(rows.shape[1] // LANES)]
    scale = jnp.zeros((GROUP, LANES), F32)
    for c in range(GROUP):
        inverse_root = lax.rsqrt(jnp.broadcast_to(columns[c][c : c + 1, :], (height, LANES)))
        scale = jnp.where(row_number[:GROUP] == c, inverse_root[:GROUP], scale)
        factor = jnp.where(row_number > c, columns[c] * (inverse_root * inverse_root), 0.0)
        for d in range(c + 1, GROUP):
            columns[d] = columns[d] - factor * jnp.broadcast_to(columns[d][c : c + 1, :], (height, LANES))
        pieces = [p - factor * jnp.broadcast_to(p[c : c + 1, :], (height, LANES)) for p in pieces]
    done = jnp.concatenate([p[:GROUP] * scale for p in pieces], axis=1)
    return done, jnp.concatenate([p[GROUP:] for p in pieces], axis=1)


def inverse_cholesky_kernel(gram_ref, out_ref, work_ref, block_ref):
    n = gram_ref.shape[0]
    rows = lax.broadcasted_iota(jnp.int32, (n, n), 0)
    columns = lax.broadcasted_iota(jnp.int32, (n, n), 1)
    work_ref[:, :n] = gram_ref[...]
    work_ref[:, n:] = jnp.where(rows == columns, 1.0, 0.0).astype(F32)

    def step(k, carry):
        at = pl.multiple_of(k * LANES, LANES)
        rows = lax.broadcasted_iota(jnp.int32, (LANES, LANES), 0)
        columns = lax.broadcasted_iota(jnp.int32, (LANES, LANES), 1)
        block_ref[:, :LANES] = work_ref[pl.ds(at, LANES), pl.ds(at, LANES)]
        block_ref[:, LANES:] = jnp.where(rows == columns, 1.0, 0.0).astype(F32)
        ahead = block_ref[:GROUP, :]
        for start in range(0, LANES, GROUP):
            end = start + GROUP
            rows = ahead if end == LANES else jnp.concatenate([ahead, block_ref[end : end + GROUP, :]], axis=0)
            done, ahead = eliminate_group(rows, start)
            block_ref[start:end, :] = done
            end += GROUP
            if end < LANES:
                block_ref[end:, :] = block_ref[end:, :] - matmul_left_t(done[:, end:LANES], done, HIGHEST)
        for lo in range(0, n, LANES):
            pl.when(k == lo // LANES)(lambda lo=lo: spread(lo))
        return carry

    def spread(lo):
        hi = lo + LANES
        panel = matmul(block_ref[:, LANES:], work_ref[lo:hi, hi : n + hi], HIGHEST)
        if hi < n:
            work_ref[hi:n, hi : n + hi] = work_ref[hi:n, hi : n + hi] - matmul_left_t(panel[:, : n - hi], panel, HIGHEST)
            out_ref[lo:hi, hi:] = jnp.zeros((LANES, n - hi), F32)
        out_ref[lo:hi, :hi] = panel[:, n - hi :]

    lax.fori_loop(0, n // LANES, step, 0)


def inverse_cholesky(gram):
    n = gram.shape[0]
    return pl.pallas_call(
        inverse_cholesky_kernel,
        out_shape=jax.ShapeDtypeStruct((n, n), F32),
        in_specs=[pl.BlockSpec(memory_space=pltpu.VMEM)],
        out_specs=pl.BlockSpec(memory_space=pltpu.VMEM),
        scratch_shapes=[pltpu.VMEM((n, 2 * n), F32), pltpu.VMEM((LANES, 2 * LANES), F32)],
        compiler_params=pltpu.CompilerParams(vmem_limit_bytes=KERNEL_BYTES),
        name="inverse_cholesky",
    )(gram)


def centre_kernel(order_ref, x_ref, average_ref, out_ref):
    for j in range(out_ref.shape[1] // LANES):
        source = pl.ds(pl.multiple_of(order_ref[j] * LANES, LANES), LANES)
        out_ref[:, j * LANES : (j + 1) * LANES] = (x_ref[:, source].astype(F32) - average_ref[:, source]).astype(BF16)


def centre(x, average, order):
    blocks = order.shape[0]
    width = x.shape[1] // blocks
    if width != LANES:
        columns = (order[:, None] * width + jnp.arange(width)).reshape(-1)
        return jnp.take((x.astype(F32) - average).astype(BF16), columns, axis=1)
    return pl.pallas_call(
        centre_kernel,
        out_shape=jax.ShapeDtypeStruct(x.shape, BF16),
        in_specs=[
            pl.BlockSpec(memory_space=pltpu.SMEM),
            pl.BlockSpec(memory_space=pltpu.VMEM),
            pl.BlockSpec(memory_space=pltpu.VMEM),
        ],
        out_specs=pl.BlockSpec(memory_space=pltpu.VMEM),
        compiler_params=pltpu.CompilerParams(vmem_limit_bytes=KERNEL_BYTES),
        name="centre",
    )(order, x, average)


def make_body(n_cluster, n_member):
    cluster_bits = [1 << b for b in range(n_cluster.bit_length() - 1)]
    member_bits = [1 << b for b in range(n_member.bit_length() - 1)]
    core = member_bits[0]
    outer = range(2 * core, n_member, 2 * core)
    orders = (cluster_bits, cluster_bits[::-1])

    def swap(x, axis, bit):
        size = n_cluster if axis == "cluster" else n_member
        return lax.ppermute(x, axis, [(i, i ^ bit) for i in range(size)])

    def with_bit(numbers, bit):
        return [i ^ bit for i in numbers]

    blocks = [0, *outer]
    parts = [blocks[: len(blocks) // 2], blocks[len(blocks) // 2 :]]
    pieces = []
    for numbers, order in zip(parts, orders):
        for bit in order[:-1]:
            numbers = numbers + with_bit(numbers, bit * n_member)
        pieces += [numbers, with_bit(numbers, order[-1] * n_member)]
    pieces = [pieces[0], pieces[2], pieces[1], pieces[3]]
    pieces += [with_bit(p, core) for p in pieces]
    relative = [i for p in pieces for i in p]

    def gather_steps(x, send):
        blocks = [x] + [send(x, "member", other) for other in outer]
        middle = len(blocks) // 2
        parts = [jnp.concatenate(blocks[:middle]), jnp.concatenate(blocks[middle:])]
        for i in range(len(cluster_bits) - 1):
            parts = [jnp.concatenate([y, send(y, "cluster", order[i])]) for y, order in zip(parts, orders)]
        held = parts + [send(y, "cluster", order[-1]) for y, order in zip(parts, orders)]
        return held + [swap(p, "member", core) for p in held]

    def reduce_steps(products, send):
        def halve(x, axis, bit, kind):
            half = x.shape[0] // 2
            return x[:half] + send(x[half:].astype(kind), axis, bit).astype(F32)

        held = [products[i] + swap(products[i + 4], "member", core) for i in range(4)]
        parts = [
            held[i] + send(held[i + 2].astype(BF16), "cluster", order[-1]).astype(F32) for i, order in enumerate(orders)
        ]
        for i in range(len(cluster_bits) - 2, -1, -1):
            parts = [halve(y, "cluster", order[i], BF16) for y, order in zip(parts, orders)]
        rows = parts[0].shape[0] // (len(blocks) // 2)
        own, *others = [y[i : i + rows] for y in parts for i in range(0, y.shape[0], rows)]
        for block, other in zip(others, outer):
            own = own + send(block.astype(BF16), "member", other).astype(F32)
        return own

    def all_sum(x, near):
        x = x + swap(x, "member", core)
        x, _ = lax.optimization_barrier((x, near))
        x = sum([swap(x, "member", other) for other in outer], x)
        return sum([swap(x, "cluster", other) for other in range(1, n_cluster)], x)

    def body(embeddings, start_basis, cluster_ids, valid_counts):
        row_count = embeddings.shape[0]
        total_rows = row_count * n_cluster * n_member
        member = lax.axis_index("member")
        own = lax.axis_index("cluster") * n_member + member
        ones_row = jnp.ones((1, row_count), BF16)
        first = []

        def first_send(x, axis, bit):
            first.append(swap(x, axis, bit))
            return first[-1]

        start_pieces = gather_steps(start_basis, first_send)
        average = all_sum(matmul(ones_row, embeddings), first[0]) / total_rows
        average, *_ = lax.optimization_barrier((average, *first[len(outer) : len(outer) + 2]))
        centered = centre(embeddings, average, own ^ jnp.array(relative, jnp.int32))
        ends = [0]
        for p in pieces:
            ends.append(ends[-1] + len(p) * start_basis.shape[0])
        centered_pieces = [centered[:, a:b] for a, b in zip(ends[:-1], ends[1:])]

        position = jnp.arange(row_count, dtype=jnp.int32)

        ids, _ = lax.optimization_barrier((cluster_ids, start_pieces[4]))
        codes = jnp.where(member * row_count + position < valid_counts[0], ids, -1)
        codes = jnp.stack([codes] + [swap(codes, "member", other) for other in outer])

        def project(basis_pieces):
            return sum(matmul(c, b) for c, b in zip(centered_pieces, basis_pieces))

        projected, codes = lax.optimization_barrier((project(start_pieces).astype(BF16), codes))
        codes = jnp.stack([codes, swap(codes, "member", core)], axis=1)
        for sweep in range(ITERS):
            products = [matmul_left_t(c, projected) for c in centered_pieces]
            image = reduce_steps(products, swap) / total_rows
            image_rounded = image.astype(BF16)
            image_pieces = gather_steps(image_rounded, swap)
            gram = sum(matmul_left_t(p, p) for p in image_pieces)
            if sweep == 0:
                gram, codes = lax.optimization_barrier((gram, codes))
            inverse = inverse_cholesky(gram)
            coords = matmul_right_t(project(image_pieces), inverse, HIGHEST)
            projected = coords.astype(BF16)
        subspace = matmul_right_t(image, inverse, HIGHEST) * math.sqrt(D)
        unit = (coords * lax.rsqrt(jnp.sum(coords * coords, axis=1, keepdims=True) + EPS)).astype(BF16)
        unit_pieces = [unit] + [swap(unit, "member", other) for other in outer]
        unit_pieces[1], subspace = lax.optimization_barrier((unit_pieces[1], subspace))
        unit_pieces += [swap(p, "member", core) for p in unit_pieces]
        nearest = jnp.full((row_count,), -1.0, F32)
        for i, other in enumerate(unit_pieces):
            scores = matmul_right_t(unit, other)
            across, block = divmod(i, len(blocks))
            allowed = cluster_ids[:, None] == codes[block, across][None, :]
            if i == 0:
                allowed = allowed & (position[:, None] != position[None, :])
            nearest = jnp.maximum(nearest, jnp.max(jnp.where(allowed, scores, -1.0), axis=1))
        return (subspace, nearest)

    return body


def solution(mesh):
    rows = ("cluster", "member")
    return jax.shard_map(
        make_body(mesh.shape["cluster"], mesh.shape["member"]),
        mesh=mesh,
        in_specs=(P(rows, None), P(rows, None), P(rows), P("cluster")),
        out_specs=(P(rows, None), P(rows)),
        check_vma=False,
    )
```

```python
import math

import jax
import jax.numpy as jnp
from jax import lax
from jax.experimental import pallas as pl
from jax.experimental.pallas import tpu as pltpu
from jax.sharding import PartitionSpec as P

D = 4096
ITERS = 2
EPS = 1e-06
HIGHEST = lax.Precision.HIGHEST
F32 = jnp.float32
BF16 = jnp.bfloat16
LANES = 128
GROUP = 16
KERNEL_BYTES = 8 << 20


def matmul(a, b, precision=None):
    return lax.dot_general(a, b, (((1,), (0,)), ((), ())), precision=precision, preferred_element_type=F32)


def matmul_left_t(a, b, precision=None):
    return lax.dot_general(a, b, (((0,), (0,)), ((), ())), precision=precision, preferred_element_type=F32)


def matmul_right_t(a, b, precision=None):
    return lax.dot_general(a, b, (((1,), (1,)), ((), ())), precision=precision, preferred_element_type=F32)


def eliminate_group(rows, at):
    height = rows.shape[0]
    columns = [jnp.broadcast_to(rows[:, at + c : at + c + 1], (height, LANES)) for c in range(GROUP)]
    row_number = lax.broadcasted_iota(jnp.int32, (height, LANES), 0)
    pieces = [rows[:, i * LANES : (i + 1) * LANES] for i in range(rows.shape[1] // LANES)]
    scale = jnp.zeros((GROUP, LANES), F32)
    for c in range(GROUP):
        inverse_root = lax.rsqrt(jnp.broadcast_to(columns[c][c : c + 1, :], (height, LANES)))
        scale = jnp.where(row_number[:GROUP] == c, inverse_root[:GROUP], scale)
        factor = jnp.where(row_number > c, columns[c] * (inverse_root * inverse_root), 0.0)
        for d in range(c + 1, GROUP):
            columns[d] = columns[d] - factor * jnp.broadcast_to(columns[d][c : c + 1, :], (height, LANES))
        pieces = [p - factor * jnp.broadcast_to(p[c : c + 1, :], (height, LANES)) for p in pieces]
    done = jnp.concatenate([p[:GROUP] * scale for p in pieces], axis=1)
    return done, jnp.concatenate([p[GROUP:] for p in pieces], axis=1)


def inverse_cholesky_kernel(gram_ref, out_ref, work_ref, block_ref):
    n = gram_ref.shape[0]
    rows = lax.broadcasted_iota(jnp.int32, (n, n), 0)
    columns = lax.broadcasted_iota(jnp.int32, (n, n), 1)
    work_ref[:, :n] = gram_ref[...]
    work_ref[:, n:] = jnp.where(rows == columns, 1.0, 0.0).astype(F32)

    def step(k, carry):
        at = pl.multiple_of(k * LANES, LANES)
        rows = lax.broadcasted_iota(jnp.int32, (LANES, LANES), 0)
        columns = lax.broadcasted_iota(jnp.int32, (LANES, LANES), 1)
        block_ref[:, :LANES] = work_ref[pl.ds(at, LANES), pl.ds(at, LANES)]
        block_ref[:, LANES:] = jnp.where(rows == columns, 1.0, 0.0).astype(F32)
        ahead = block_ref[:GROUP, :]
        for start in range(0, LANES, GROUP):
            end = start + GROUP
            rows = ahead if end == LANES else jnp.concatenate([ahead, block_ref[end : end + GROUP, :]], axis=0)
            done, ahead = eliminate_group(rows, start)
            block_ref[start:end, :] = done
            end += GROUP
            if end < LANES:
                block_ref[end:, :] = block_ref[end:, :] - matmul_left_t(done[:, end:LANES], done, HIGHEST)
        for lo in range(0, n, LANES):
            pl.when(k == lo // LANES)(lambda lo=lo: spread(lo))
        return carry

    def spread(lo):
        hi = lo + LANES
        panel = matmul(block_ref[:, LANES:], work_ref[lo:hi, hi : n + hi], HIGHEST)
        if hi < n:
            work_ref[hi:n, hi : n + hi] = work_ref[hi:n, hi : n + hi] - matmul_left_t(panel[:, : n - hi], panel, HIGHEST)
            out_ref[lo:hi, hi:] = jnp.zeros((LANES, n - hi), F32)
        out_ref[lo:hi, :hi] = panel[:, n - hi :]

    lax.fori_loop(0, n // LANES, step, 0)


def inverse_cholesky(gram):
    n = gram.shape[0]
    return pl.pallas_call(
        inverse_cholesky_kernel,
        out_shape=jax.ShapeDtypeStruct((n, n), F32),
        in_specs=[pl.BlockSpec(memory_space=pltpu.VMEM)],
        out_specs=pl.BlockSpec(memory_space=pltpu.VMEM),
        scratch_shapes=[pltpu.VMEM((n, 2 * n), F32), pltpu.VMEM((LANES, 2 * LANES), F32)],
        compiler_params=pltpu.CompilerParams(vmem_limit_bytes=KERNEL_BYTES),
        name="inverse_cholesky",
    )(gram)


def centre_kernel(order_ref, x_ref, average_ref, out_ref):
    for j in range(out_ref.shape[1] // LANES):
        source = pl.ds(pl.multiple_of(order_ref[j] * LANES, LANES), LANES)
        out_ref[:, j * LANES : (j + 1) * LANES] = (x_ref[:, source].astype(F32) - average_ref[:, source]).astype(BF16)


def centre(x, average, order):
    blocks = order.shape[0]
    width = x.shape[1] // blocks
    if width != LANES:
        columns = (order[:, None] * width + jnp.arange(width)).reshape(-1)
        return jnp.take((x.astype(F32) - average).astype(BF16), columns, axis=1)
    return pl.pallas_call(
        centre_kernel,
        out_shape=jax.ShapeDtypeStruct(x.shape, BF16),
        in_specs=[
            pl.BlockSpec(memory_space=pltpu.SMEM),
            pl.BlockSpec(memory_space=pltpu.VMEM),
            pl.BlockSpec(memory_space=pltpu.VMEM),
        ],
        out_specs=pl.BlockSpec(memory_space=pltpu.VMEM),
        compiler_params=pltpu.CompilerParams(vmem_limit_bytes=KERNEL_BYTES),
        name="centre",
    )(order, x, average)


def make_body(n_cluster, n_member):
    cluster_bits = [1 << b for b in range(n_cluster.bit_length() - 1)]
    member_bits = [1 << b for b in range(n_member.bit_length() - 1)]
    core = member_bits[0]
    outer = range(2 * core, n_member, 2 * core)
    orders = (cluster_bits, cluster_bits[::-1])

    def swap(x, axis, bit):
        size = n_cluster if axis == "cluster" else n_member
        return lax.ppermute(x, axis, [(i, i ^ bit) for i in range(size)])

    def with_bit(numbers, bit):
        return [i ^ bit for i in numbers]

    blocks = [0, *outer]
    parts = [blocks[: len(blocks) // 2], blocks[len(blocks) // 2 :]]
    pieces = []
    for numbers, order in zip(parts, orders):
        for bit in order[:-1]:
            numbers = numbers + with_bit(numbers, bit * n_member)
        pieces += [numbers, with_bit(numbers, order[-1] * n_member)]
    pieces = [pieces[0], pieces[2], pieces[1], pieces[3]]
    pieces += [with_bit(p, core) for p in pieces]
    relative = [i for p in pieces for i in p]

    def gather_steps(x, send):
        blocks = [x] + [send(x, "member", other) for other in outer[::-1]][::-1]
        middle = len(blocks) // 2
        parts = [jnp.concatenate(blocks[:middle]), jnp.concatenate(blocks[middle:])]
        for i in range(len(cluster_bits) - 1):
            parts = [jnp.concatenate([y, send(y, "cluster", order[i])]) for y, order in zip(parts, orders)]
        held = parts + [send(y, "cluster", order[-1]) for y, order in zip(parts, orders)]
        return held + [swap(p, "member", core) for p in held]

    def reduce_steps(products, send):
        def halve(x, axis, bit, kind):
            half = x.shape[0] // 2
            return x[:half] + send(x[half:].astype(kind), axis, bit).astype(F32)

        held = [products[i] + swap(products[i + 4], "member", core) for i in range(4)]
        parts = [
            held[i] + send(held[i + 2].astype(BF16), "cluster", order[-1]).astype(F32) for i, order in enumerate(orders)
        ]
        for i in range(len(cluster_bits) - 2, -1, -1):
            parts = [halve(y, "cluster", order[i], BF16) for y, order in zip(parts, orders)]
        rows = parts[0].shape[0] // (len(blocks) // 2)
        own, *others = [y[i : i + rows] for y in parts for i in range(0, y.shape[0], rows)]
        for block, other in zip(others, outer):
            own = own + send(block.astype(BF16), "member", other).astype(F32)
        return own

    def all_sum(x, near, far):
        x = x + swap(x, "member", core)
        x, _ = lax.optimization_barrier((x, near))
        x = sum([swap(x, "member", other) for other in outer], x)
        x, *_ = lax.optimization_barrier((x, *far))
        return sum([swap(x, "cluster", other) for other in range(1, n_cluster)], x)

    def body(embeddings, start_basis, cluster_ids, valid_counts):
        row_count = embeddings.shape[0]
        total_rows = row_count * n_cluster * n_member
        member = lax.axis_index("member")
        own = lax.axis_index("cluster") * n_member + member
        ones_row = jnp.ones((1, row_count), BF16)
        first = []

        def first_send(x, axis, bit):
            first.append(swap(x, axis, bit))
            return first[-1]

        start_pieces = gather_steps(start_basis, first_send)
        average = all_sum(matmul(ones_row, embeddings), first[len(outer) - 1], first[len(outer) : len(outer) + 2]) / total_rows
        centered = centre(embeddings, average, own ^ jnp.array(relative, jnp.int32))
        ends = [0]
        for p in pieces:
            ends.append(ends[-1] + len(p) * start_basis.shape[0])
        centered_pieces = [centered[:, a:b] for a, b in zip(ends[:-1], ends[1:])]

        position = jnp.arange(row_count, dtype=jnp.int32)

        ids, _ = lax.optimization_barrier((cluster_ids, start_pieces[4]))
        codes = jnp.where(member * row_count + position < valid_counts[0], ids, -1)
        codes = jnp.stack([codes] + [swap(codes, "member", other) for other in outer])

        def project(basis_pieces):
            return sum(matmul(c, b) for c, b in zip(centered_pieces, basis_pieces))

        projected, codes = lax.optimization_barrier((project(start_pieces).astype(BF16), codes))
        codes = jnp.stack([codes, swap(codes, "member", core)], axis=1)
        for sweep in range(ITERS):
            products = [matmul_left_t(c, projected) for c in centered_pieces]
            image = reduce_steps(products, swap) / total_rows
            image_rounded = image.astype(BF16)
            image_pieces = gather_steps(image_rounded, swap)
            gram = sum(matmul_left_t(p, p) for p in image_pieces)
            if sweep == 0:
                gram, codes = lax.optimization_barrier((gram, codes))
            inverse = inverse_cholesky(gram)
            coords = matmul_right_t(project(image_pieces), inverse, HIGHEST)
            projected = coords.astype(BF16)
        subspace = matmul_right_t(image, inverse, HIGHEST) * math.sqrt(D)
        unit = (coords * lax.rsqrt(jnp.sum(coords * coords, axis=1, keepdims=True) + EPS)).astype(BF16)
        unit_pieces = [unit] + [swap(unit, "member", other) for other in outer[::-1]][::-1]
        unit_pieces[1], subspace = lax.optimization_barrier((unit_pieces[1], subspace))
        unit_pieces += [swap(p, "member", core) for p in unit_pieces]
        nearest = jnp.full((row_count,), -1.0, F32)
        for i, other in enumerate(unit_pieces):
            scores = matmul_right_t(unit, other)
            across, block = divmod(i, len(blocks))
            allowed = cluster_ids[:, None] == codes[block, across][None, :]
            if i == 0:
                allowed = allowed & (position[:, None] != position[None, :])
            nearest = jnp.maximum(nearest, jnp.max(jnp.where(allowed, scores, -1.0), axis=1))
        return (subspace, nearest)

    return body


def solution(mesh):
    rows = ("cluster", "member")
    return jax.shard_map(
        make_body(mesh.shape["cluster"], mesh.shape["member"]),
        mesh=mesh,
        in_specs=(P(rows, None), P(rows, None), P(rows), P("cluster")),
        out_specs=(P(rows, None), P(rows)),
        check_vma=False,
    )
```

```python
import math

import jax
import jax.numpy as jnp
from jax import lax
from jax.experimental import pallas as pl
from jax.experimental.pallas import tpu as pltpu
from jax.sharding import PartitionSpec as P

D = 4096
ITERS = 2
EPS = 1e-06
HIGHEST = lax.Precision.HIGHEST
F32 = jnp.float32
BF16 = jnp.bfloat16
LANES = 128
GROUP = 16
KERNEL_BYTES = 8 << 20


def matmul(a, b, precision=None):
    return lax.dot_general(a, b, (((1,), (0,)), ((), ())), precision=precision, preferred_element_type=F32)


def matmul_left_t(a, b, precision=None):
    return lax.dot_general(a, b, (((0,), (0,)), ((), ())), precision=precision, preferred_element_type=F32)


def matmul_right_t(a, b, precision=None):
    return lax.dot_general(a, b, (((1,), (1,)), ((), ())), precision=precision, preferred_element_type=F32)


def eliminate_group(rows, at):
    height = rows.shape[0]
    columns = [jnp.broadcast_to(rows[:, at + c : at + c + 1], (height, LANES)) for c in range(GROUP)]
    row_number = lax.broadcasted_iota(jnp.int32, (height, LANES), 0)
    pieces = [rows[:, i * LANES : (i + 1) * LANES] for i in range(rows.shape[1] // LANES)]
    scale = jnp.zeros((GROUP, LANES), F32)
    for c in range(GROUP):
        inverse_root = lax.rsqrt(jnp.broadcast_to(columns[c][c : c + 1, :], (height, LANES)))
        scale = jnp.where(row_number[:GROUP] == c, inverse_root[:GROUP], scale)
        factor = jnp.where(row_number > c, columns[c] * (inverse_root * inverse_root), 0.0)
        for d in range(c + 1, GROUP):
            columns[d] = columns[d] - factor * jnp.broadcast_to(columns[d][c : c + 1, :], (height, LANES))
        pieces = [p - factor * jnp.broadcast_to(p[c : c + 1, :], (height, LANES)) for p in pieces]
    done = jnp.concatenate([p[:GROUP] * scale for p in pieces], axis=1)
    return done, jnp.concatenate([p[GROUP:] for p in pieces], axis=1)


def inverse_cholesky_kernel(gram_ref, out_ref, work_ref, block_ref):
    n = gram_ref.shape[0]
    rows = lax.broadcasted_iota(jnp.int32, (n, n), 0)
    columns = lax.broadcasted_iota(jnp.int32, (n, n), 1)
    work_ref[:, :n] = gram_ref[...]
    work_ref[:, n:] = jnp.where(rows == columns, 1.0, 0.0).astype(F32)

    def step(k, carry):
        at = pl.multiple_of(k * LANES, LANES)
        rows = lax.broadcasted_iota(jnp.int32, (LANES, LANES), 0)
        columns = lax.broadcasted_iota(jnp.int32, (LANES, LANES), 1)
        block_ref[:, :LANES] = work_ref[pl.ds(at, LANES), pl.ds(at, LANES)]
        block_ref[:, LANES:] = jnp.where(rows == columns, 1.0, 0.0).astype(F32)
        ahead = block_ref[:GROUP, :]
        for start in range(0, LANES, GROUP):
            end = start + GROUP
            rows = ahead if end == LANES else jnp.concatenate([ahead, block_ref[end : end + GROUP, :]], axis=0)
            done, ahead = eliminate_group(rows, start)
            block_ref[start:end, :] = done
            end += GROUP
            if end < LANES:
                block_ref[end:, :] = block_ref[end:, :] - matmul_left_t(done[:, end:LANES], done, HIGHEST)
        for lo in range(0, n, LANES):
            pl.when(k == lo // LANES)(lambda lo=lo: spread(lo))
        return carry

    def spread(lo):
        hi = lo + LANES
        panel = matmul(block_ref[:, LANES:], work_ref[lo:hi, hi : n + hi], HIGHEST)
        if hi < n:
            work_ref[hi:n, hi : n + hi] = work_ref[hi:n, hi : n + hi] - matmul_left_t(panel[:, : n - hi], panel, HIGHEST)
            out_ref[lo:hi, hi:] = jnp.zeros((LANES, n - hi), F32)
        out_ref[lo:hi, :hi] = panel[:, n - hi :]

    lax.fori_loop(0, n // LANES, step, 0)


def inverse_cholesky(gram):
    n = gram.shape[0]
    return pl.pallas_call(
        inverse_cholesky_kernel,
        out_shape=jax.ShapeDtypeStruct((n, n), F32),
        in_specs=[pl.BlockSpec(memory_space=pltpu.VMEM)],
        out_specs=pl.BlockSpec(memory_space=pltpu.VMEM),
        scratch_shapes=[pltpu.VMEM((n, 2 * n), F32), pltpu.VMEM((LANES, 2 * LANES), F32)],
        compiler_params=pltpu.CompilerParams(vmem_limit_bytes=KERNEL_BYTES),
        name="inverse_cholesky",
    )(gram)


def centre_kernel(order_ref, x_ref, average_ref, out_ref):
    for j in range(out_ref.shape[1] // LANES):
        source = pl.ds(pl.multiple_of(order_ref[j] * LANES, LANES), LANES)
        out_ref[:, j * LANES : (j + 1) * LANES] = (x_ref[:, source].astype(F32) - average_ref[:, source]).astype(BF16)


def centre(x, average, order):
    blocks = order.shape[0]
    width = x.shape[1] // blocks
    if width != LANES:
        columns = (order[:, None] * width + jnp.arange(width)).reshape(-1)
        return jnp.take((x.astype(F32) - average).astype(BF16), columns, axis=1)
    return pl.pallas_call(
        centre_kernel,
        out_shape=jax.ShapeDtypeStruct(x.shape, BF16),
        in_specs=[
            pl.BlockSpec(memory_space=pltpu.SMEM),
            pl.BlockSpec(memory_space=pltpu.VMEM),
            pl.BlockSpec(memory_space=pltpu.VMEM),
        ],
        out_specs=pl.BlockSpec(memory_space=pltpu.VMEM),
        compiler_params=pltpu.CompilerParams(vmem_limit_bytes=KERNEL_BYTES),
        name="centre",
    )(order, x, average)


def make_body(n_cluster, n_member):
    cluster_bits = [1 << b for b in range(n_cluster.bit_length() - 1)]
    member_bits = [1 << b for b in range(n_member.bit_length() - 1)]
    core = member_bits[0]
    outer = range(2 * core, n_member, 2 * core)
    orders = (cluster_bits, cluster_bits[::-1])

    def swap(x, axis, bit):
        size = n_cluster if axis == "cluster" else n_member
        return lax.ppermute(x, axis, [(i, i ^ bit) for i in range(size)])

    def with_bit(numbers, bit):
        return [i ^ bit for i in numbers]

    blocks = [0, *outer]
    parts = [blocks[: len(blocks) // 2], blocks[len(blocks) // 2 :]]
    pieces = []
    for numbers, order in zip(parts, orders):
        for bit in order[:-1]:
            numbers = numbers + with_bit(numbers, bit * n_member)
        pieces += [numbers, with_bit(numbers, order[-1] * n_member)]
    pieces = [pieces[0], pieces[2], pieces[1], pieces[3]]
    pieces += [with_bit(p, core) for p in pieces]
    relative = [i for p in pieces for i in p]

    def gather_steps(x, send):
        blocks = [x] + [send(x, "member", other) for other in outer[::-1]][::-1]
        middle = len(blocks) // 2
        parts = [jnp.concatenate(blocks[:middle]), jnp.concatenate(blocks[middle:])]
        for i in range(len(cluster_bits) - 1):
            parts = [jnp.concatenate([y, send(y, "cluster", order[i])]) for y, order in zip(parts, orders)]
        held = parts + [send(y, "cluster", order[-1]) for y, order in zip(parts, orders)]
        return held + [swap(p, "member", core) for p in held]

    def reduce_steps(products, send):
        def halve(x, axis, bit, kind):
            half = x.shape[0] // 2
            return x[:half] + send(x[half:].astype(kind), axis, bit).astype(F32)

        held = [products[i] + swap(products[i + 4], "member", core) for i in range(4)]
        parts = [
            held[i] + send(held[i + 2].astype(BF16), "cluster", order[-1]).astype(F32) for i, order in enumerate(orders)
        ]
        for i in range(len(cluster_bits) - 2, -1, -1):
            parts = [halve(y, "cluster", order[i], BF16) for y, order in zip(parts, orders)]
        rows = parts[0].shape[0] // (len(blocks) // 2)
        own, *others = [y[i : i + rows] for y in parts for i in range(0, y.shape[0], rows)]
        for block, other in zip(others, outer):
            own = own + send(block.astype(BF16), "member", other).astype(F32)
        return own

    def all_sum(x, near, far):
        x = x + swap(x, "member", core)
        x, _ = lax.optimization_barrier((x, near))
        x = sum([swap(x, "member", other) for other in outer[::-1]], x)
        x, *_ = lax.optimization_barrier((x, *far))
        return sum([swap(x, "cluster", other) for other in range(1, n_cluster)], x)

    def body(embeddings, start_basis, cluster_ids, valid_counts):
        row_count = embeddings.shape[0]
        total_rows = row_count * n_cluster * n_member
        member = lax.axis_index("member")
        own = lax.axis_index("cluster") * n_member + member
        ones_row = jnp.ones((1, row_count), BF16)
        first = []

        def first_send(x, axis, bit):
            first.append(swap(x, axis, bit))
            return first[-1]

        start_pieces = gather_steps(start_basis, first_send)
        average = all_sum(matmul(ones_row, embeddings), first[len(outer) - 1], first[len(outer) : len(outer) + 2]) / total_rows
        centered = centre(embeddings, average, own ^ jnp.array(relative, jnp.int32))
        ends = [0]
        for p in pieces:
            ends.append(ends[-1] + len(p) * start_basis.shape[0])
        centered_pieces = [centered[:, a:b] for a, b in zip(ends[:-1], ends[1:])]

        position = jnp.arange(row_count, dtype=jnp.int32)

        ids, _ = lax.optimization_barrier((cluster_ids, start_pieces[4]))
        codes = jnp.where(member * row_count + position < valid_counts[0], ids, -1)
        codes = jnp.stack([codes] + [swap(codes, "member", other) for other in outer[::-1]][::-1])

        def project(basis_pieces):
            return sum(matmul(c, b) for c, b in zip(centered_pieces, basis_pieces))

        projected, codes = lax.optimization_barrier((project(start_pieces).astype(BF16), codes))
        codes = jnp.stack([codes, swap(codes, "member", core)], axis=1)
        for sweep in range(ITERS):
            products = [matmul_left_t(c, projected) for c in centered_pieces]
            image = reduce_steps(products, swap) / total_rows
            image_rounded = image.astype(BF16)
            image_pieces = gather_steps(image_rounded, swap)
            gram = sum(matmul_left_t(p, p) for p in image_pieces)
            if sweep == 0:
                gram, codes = lax.optimization_barrier((gram, codes))
            inverse = inverse_cholesky(gram)
            coords = matmul_right_t(project(image_pieces), inverse, HIGHEST)
            projected = coords.astype(BF16)
        subspace = matmul_right_t(image, inverse, HIGHEST) * math.sqrt(D)
        unit = (coords * lax.rsqrt(jnp.sum(coords * coords, axis=1, keepdims=True) + EPS)).astype(BF16)
        unit_pieces = [unit] + [swap(unit, "member", other) for other in outer[::-1]][::-1]
        unit_pieces[1], subspace = lax.optimization_barrier((unit_pieces[1], subspace))
        unit_pieces += [swap(p, "member", core) for p in unit_pieces]
        nearest = jnp.full((row_count,), -1.0, F32)
        for i, other in enumerate(unit_pieces):
            scores = matmul_right_t(unit, other)
            across, block = divmod(i, len(blocks))
            allowed = cluster_ids[:, None] == codes[block, across][None, :]
            if i == 0:
                allowed = allowed & (position[:, None] != position[None, :])
            nearest = jnp.maximum(nearest, jnp.max(jnp.where(allowed, scores, -1.0), axis=1))
        return (subspace, nearest)

    return body


def solution(mesh):
    rows = ("cluster", "member")
    return jax.shard_map(
        make_body(mesh.shape["cluster"], mesh.shape["member"]),
        mesh=mesh,
        in_specs=(P(rows, None), P(rows, None), P(rows), P("cluster")),
        out_specs=(P(rows, None), P(rows)),
        check_vma=False,
    )
```
